32 devices in a mesh: cp: 4 (over z), dp: 8 (over y, x, core).
Axes of the slice: x: 2, y: 2, z: 4, core: 2. Of those that a mesh axis runs over, the one named last changes fastest.
Arguments:
- tokens: bfloat16 [32, 1536, 7168], P('dp', 'cp')
- choices: int32 [32, 1536, 8], P('dp', 'cp')
- router_w: float32 [384, 7168], replicated
- expert_bias: float32 [384], replicated
Outputs:
- output 1: float32 [], replicated
- output 2: float32 [384, 7168], replicated
- output 3: bfloat16 [32, 1536, 7168], P('dp', 'cp')
- output 4: float32 [384], replicated
All inputs are finite; a program needn't handle non-finite values.
Results may differ from the reference program's by a relative error of at most 0.001.
Values sent between devices are 32-bit elements.
A program may use at most 1 GiB of HBM per device.

```python
import jax
import jax.numpy as jnp
from jax import lax

ROWS = 32
SEQ = 1536
EXPERTS = 384
TOP = 8
DIM = 7168
ALPHA = 0.1
GAMMA = 0.001


def draw_choices(route_key, glob_key, seq_key):
    noise = jax.random.randint(route_key, (ROWS, SEQ, EXPERTS), 0, 1024)
    glob_pref = jax.random.randint(glob_key, (EXPERTS,), 0, 768)
    seq_pref = jax.random.randint(seq_key, (ROWS, 1, EXPERTS), 0, 512)
    score = (noise + glob_pref + seq_pref) * EXPERTS + jnp.arange(EXPERTS, dtype=jnp.int32)
    return lax.top_k(score, TOP)[1].astype(jnp.int32)


def setup_inputs(seed: int = 0) -> dict:
    root_key = jax.random.key(seed)
    tok_key, route_key, glob_key, seq_key, gate_key, bias_key = jax.random.split(root_key, 6)
    tokens = jax.random.normal(tok_key, (ROWS, SEQ, DIM), jnp.float32).astype(jnp.bfloat16)
    choices = draw_choices(route_key, glob_key, seq_key)
    router_w = jax.random.normal(gate_key, (EXPERTS, DIM), jnp.float32) * (DIM ** -0.5)
    expert_bias = jax.random.normal(bias_key, (EXPERTS,), jnp.float32) * GAMMA
    return {"tokens": tokens, "choices": choices, "router_w": router_w, "expert_bias": expert_bias}


def reference(tokens, choices, router_w, expert_bias):
    expert_ids = jnp.arange(EXPERTS, dtype=jnp.int32)

    def seq_step(carry, row):
        row_tok, row_choice = row
        counts = jnp.sum((row_choice[:, :, None] == expert_ids).astype(jnp.float32), axis=(0, 1))
        load_frac = counts * (EXPERTS / (TOP * SEQ))

        def seq_loss(weights, toks):
            logits = jnp.dot(toks, weights.T, preferred_element_type=jnp.float32)
            sig_probs = jax.nn.sigmoid(logits)
            normed = sig_probs / jnp.sum(sig_probs, axis=-1, keepdims=True)
            mean_prob = jnp.mean(normed, axis=0)
            return jnp.sum(load_frac * mean_prob) * (ALPHA / ROWS)

        loss_val, pull_back = jax.vjp(seq_loss, router_w, row_tok.astype(jnp.float32))
        grad_w, grad_x = pull_back(jnp.ones_like(loss_val))
        new_carry = (carry[0] + grad_w, carry[1] + loss_val)
        return new_carry, (grad_x.astype(jnp.bfloat16), counts)

    init = (jnp.zeros((EXPERTS, DIM), jnp.float32), jnp.zeros((), jnp.float32))
    (grad_router, bal_loss), (grad_tokens, counts) = lax.scan(seq_step, init, (tokens, choices))
    global_load = jnp.sum(counts, axis=0)
    load_gap = ROWS * SEQ * TOP - EXPERTS * global_load.astype(jnp.int32)
    new_bias = expert_bias + GAMMA * jnp.sign(load_gap).astype(jnp.float32)
    return bal_loss, grad_router, grad_tokens, new_bias
```

```python
import functools

import jax
import jax.numpy as jnp
from jax import lax
from jax.experimental import pallas as pl
from jax.experimental.pallas import tpu as pltpu
from jax.sharding import PartitionSpec as P

ALPHA = 0.1
GAMMA = 0.001
MESH = pl.DeviceIdType.MESH
ANY = pl.BlockSpec(memory_space=pl.ANY)
VMEM = pl.BlockSpec(memory_space=pltpu.VMEM)
COLS = 512
LEVELS = 5
WAIT_RS = (2, 4, 6, 8, 10)
WAIT_AG = (20, 18, 16, 14, 12)


def pieces(val):
    hi = val.astype(jnp.bfloat16)
    rest = val - hi.astype(jnp.float32)
    mid = rest.astype(jnp.bfloat16)
    low = (rest - mid.astype(jnp.float32)).astype(jnp.bfloat16)
    return hi, mid, low


def weight_stack(w, stack, order=(0, 1, 0, 2, 1, 0)):
    experts = w.shape[0]
    parts = pieces(w)
    for k, which in enumerate(order):
        stack[pl.ds(k * experts, experts), :] = parts[which]


def main_kernel(n_dx, seqs, scale, cnt_ref, x_ref, w_ref, dw_ref, dx_ref, cols_out, small_out,
                acc, full, got0, got1, got2, got3, got4, xbuf, wbuf, stack, scores, rows_ref, cols_ref,
                cnt_cur, cnt_got, small_cur, small_got,
                rs_send, rs_recv, ag_send, ag_recv, sm_send, sm_recv, cnt_send, cnt_recv,
                x_sem, w_sem, o_sem, d_sem, c_sem):
    n_chunk, experts = acc.shape[0], acc.shape[1]
    tok_n = xbuf.shape[1]
    seq = tok_n // seqs
    z, dp = lax.axis_index("cp"), lax.axis_index("dp")
    core, xb, yb = dp % 2, (dp // 2) % 2, dp // 4
    zl, zh = z % 2, z // 2
    by_core = (z, dp + 1 - 2 * core)
    by_x = (z, dp + 2 - 4 * xb)
    by_y = (z, dp + 4 - 8 * yb)
    by_zl = (z + 1 - 2 * zl, dp)
    by_zh = (z + 2 - 4 * zh, dp)
    first = (z, dp + (1 - core) * (2 - 4 * xb) + core * (4 - 8 * yb))
    second = (z, dp + core * (2 - 4 * xb) + (1 - core) * (4 - 8 * yb))
    peers = (by_core, first, by_zl, second, by_zh)
    bits = (core, (1 - core) * xb + core * yb, zl, (1 - core) * yb + core * xb, zh)
    got = (got0, got1, got2, got3, got4)

    barrier = pltpu.get_barrier_semaphore()
    for peer in (by_core, by_x, by_y, by_zl, by_zh):
        pl.semaphore_signal(barrier, inc=1, device_id=peer, device_id_type=MESH)

    size, keep, away, base = experts, [], [], 0
    for level in range(LEVELS - 1):
        size //= 2
        keep.append((pl.multiple_of(base + bits[level] * size, 8), size, 0, COLS))
        away.append((pl.multiple_of(base + (1 - bits[level]) * size, 8), size, 0, COLS))
        base = base + bits[level] * size
    half = COLS // 2
    row = pl.multiple_of(base, 8)
    keep.append((row, size, pl.multiple_of(zh * half, 128), half))
    away.append((row, size, pl.multiple_of((1 - zh) * half, 128), half))

    def region(ref, c, where):
        r, n, k, m = where
        return ref.at[c, pl.ds(r, n), pl.ds(k, m)]

    def rs_copy(level, c):
        return pltpu.make_async_remote_copy(
            src_ref=region(acc, c, away[level]), dst_ref=got[level].at[c], send_sem=rs_send.at[level, c],
            recv_sem=rs_recv.at[level, c], device_id=peers[level], device_id_type=MESH)

    def ag_copy(level, c):
        return pltpu.make_async_remote_copy(
            src_ref=region(full, c, keep[level]), dst_ref=region(full, c, keep[level]), send_sem=ag_send.at[level, c],
            recv_sem=ag_recv.at[level, c], device_id=peers[level], device_id_type=MESH)

    def sm_copy(level):
        return pltpu.make_async_remote_copy(
            src_ref=small_cur.at[level], dst_ref=small_got.at[level], send_sem=sm_send.at[level],
            recv_sem=sm_recv.at[level], device_id=(by_core, by_x, by_zl, by_y, by_zh)[level],
            device_id_type=MESH)

    def cnt_copy(k):
        return pltpu.make_async_remote_copy(
            src_ref=cnt_cur.at[k], dst_ref=cnt_got.at[k], send_sem=cnt_send.at[k],
            recv_sem=cnt_recv.at[k], device_id=(by_zl, by_zh)[k], device_id_type=MESH)

    def x_load(c):
        return pltpu.make_async_copy(
            x_ref.at[:, pl.ds(pl.multiple_of(c * COLS, COLS), COLS)], xbuf.at[c % 2], x_sem.at[c % 2])

    def w_load(j):
        return pltpu.make_async_copy(
            w_ref.at[:, pl.ds(pl.multiple_of(j * COLS, COLS), COLS)], wbuf.at[j % 2], w_sem.at[j % 2])

    def dx_store(j):
        return pltpu.make_async_copy(xbuf.at[j % 2], dx_ref.at[j], o_sem.at[j % 2])

    def dw_store(c):
        return pltpu.make_async_copy(full.at[c], dw_ref.at[c], d_sem.at[c])

    x_load(0).start()
    x_load(1).start()
    w_load(0).start()
    w_load(1).start()
    cnt_cur[0] = cnt_ref[...]
    scores[...] = jnp.zeros_like(scores)
    pl.semaphore_wait(barrier, LEVELS)
    cnt_copy(0).start()

    def score_step(i, carry):
        w_load(i).wait()
        weight_stack(wbuf[i % 2], stack, (0, 1, 2))
        x_load(i).wait()
        for t in range(0, tok_n, COLS):
            out = lax.dot_general(
                stack[pl.ds(0, 3 * experts), :], xbuf[i % 2, pl.ds(t, COLS), :], (((1,), (1,)), ((), ())),
                preferred_element_type=jnp.float32)
            scores[:, pl.ds(t, COLS)] += out[:experts] + (out[experts:2 * experts] + out[2 * experts:])
        after = (i + 2) % n_chunk
        x_load(after).start()
        w_load(after).start()

        @pl.when(i == n_chunk // 2)
        def _():
            cnt_copy(0).wait_send()
            cnt_copy(0).wait_recv()
            cnt_cur[1] = cnt_cur[0] + cnt_got[0]
            cnt_copy(1).start()

        return carry

    lax.fori_loop(0, n_chunk, score_step, 0)
    cnt_copy(1).wait_send()
    cnt_copy(1).wait_recv()
    cnt_cur[2] = cnt_cur[1] + cnt_got[1]
    small_cur[0] = jnp.zeros_like(small_cur[0])

    def grad_step(r, carry):
        span = pl.ds(pl.multiple_of(r * seq, seq), seq)
        place = lax.broadcasted_iota(jnp.int32, (experts, experts), 0)
        diag = place == lax.broadcasted_iota(jnp.int32, (experts, experts), 1)
        weight = jnp.sum(jnp.where(diag, cnt_cur[2, pl.ds(r, 1), :], 0.0), axis=1, keepdims=True) * scale
        sig = jax.nn.sigmoid(scores[:, span])
        total = jnp.sum(sig, axis=0, keepdims=True)
        normed = sig / total
        mixed = jnp.sum(normed * weight, axis=0, keepdims=True)
        grad = (weight - mixed) * (sig * (1.0 - sig) / total)
        for k, part in enumerate(pieces(grad)):
            rows_ref[pl.ds(k * experts, experts), span] = part
        turned = pieces(grad.T)
        for k, which in enumerate((0, 0, 1, 0, 1, 2)):
            cols_ref[span, pl.ds(k * experts, experts)] = turned[which]
        loss = jnp.sum(mixed, axis=1, keepdims=True)
        row_id = lax.broadcasted_iota(jnp.int32, (8, experts), 0)
        loads = cnt_ref[pl.ds(r, 1), :]
        small_cur[0] += jnp.where(row_id == 0, loads, jnp.where(row_id == 1, loss, 0.0))
        return carry

    lax.fori_loop(0, seqs, grad_step, 0)
    cols_copy = pltpu.make_async_copy(cols_ref, cols_out, c_sem)
    cols_copy.start()

    def step(i, carry):
        def at(offset):
            c = i - offset
            return c, jnp.logical_and(c >= 0, c < n_chunk)

        for level in range(LEVELS):
            c, live = at(WAIT_AG[level])

            @pl.when(live)
            def _(level=level, c=c):
                copy = ag_copy(level, c)
                copy.wait_send()
                copy.wait_recv()
                if level > 0:
                    ag_copy(level - 1, c).start()
                else:
                    dw_store(c).start()

        for level in reversed(range(LEVELS)):
            c, live = at(WAIT_RS[level])

            @pl.when(live)
            def _(level=level, c=c):
                copy = rs_copy(level, c)
                copy.wait_send()
                copy.wait_recv()
                r, n, k, m = keep[level]
                total = acc[c, pl.ds(r, n), pl.ds(k, m)] + got[level][c]
                if level < LEVELS - 1:
                    acc[c, pl.ds(r, n), pl.ds(k, m)] = total
                    rs_copy(level + 1, c).start()
                else:
                    full[c, pl.ds(r, n), pl.ds(k, m)] = total
                    ag_copy(level, c).start()

        for level in range(LEVELS + 1):
            @pl.when(i == 2 * level)
            def _(level=level):
                if level > 0:
                    copy = sm_copy(level - 1)
                    copy.wait_send()
                    copy.wait_recv()
                    total = small_cur[level - 1] + small_got[level - 1]
                    if level < LEVELS:
                        small_cur[level] = total
                    else:
                        small_out[...] = total
                if level < LEVELS:
                    sm_copy(level).start()

        @pl.when(i < n_chunk)
        def _():
            x_load(i).wait()
            out = jnp.dot(rows_ref[...], xbuf[i % 2], preferred_element_type=jnp.float32)
            acc[i] = out[:experts] + (out[experts:2 * experts] + out[2 * experts:])
            rs_copy(0, i).start()

            @pl.when(i + 2 < n_chunk)
            def _():
                x_load(i + 2).start()

        @pl.when(jnp.logical_and(i >= n_chunk, i < n_chunk + n_dx))
        def _():
            j = i - n_chunk
            w_load(j).wait()
            weight_stack(wbuf[j % 2], stack)

            @pl.when(j + 2 < n_dx)
            def _():
                w_load(j + 2).start()

            @pl.when(j >= 2)
            def _():
                dx_store(j - 2).wait()

            xbuf[j % 2] = jnp.dot(
                cols_ref[...], stack[...], preferred_element_type=jnp.float32).astype(jnp.bfloat16)
            dx_store(j).start()

        return carry

    lax.fori_loop(0, n_chunk + WAIT_AG[0], step, 0)
    dx_store(n_dx - 2).wait()
    dx_store(n_dx - 1).wait()

    def finish(c, carry):
        dw_store(c).wait()
        return carry

    lax.fori_loop(0, n_chunk, finish, 0)
    cols_copy.wait()


def last_kernel(cols_ref, w_ref, dw_in, dx_in, dw_ref, dx_ref,
                wbuf, stack, obuf, dwbuf, dxbuf, w_sem, o_sem, dwi, dwo, dxi, dxo):
    n_chunk, n_done = dw_in.shape[0], dx_in.shape[0]
    n_left = n_chunk - n_done

    def cols(c):
        return pl.ds(pl.multiple_of(c * COLS, COLS), COLS)

    def w_load(j):
        return pltpu.make_async_copy(w_ref.at[:, cols(n_done + j)], wbuf.at[j], w_sem.at[j])

    def dw_load(c):
        return pltpu.make_async_copy(dw_in.at[c], dwbuf.at[c], dwi.at[c])

    def dw_store(c):
        return pltpu.make_async_copy(dwbuf.at[c], dw_ref.at[:, cols(c)], dwo.at[c])

    def dx_load(c):
        return pltpu.make_async_copy(dx_in.at[c], dxbuf.at[c], dxi.at[c])

    def dx_move(c):
        return pltpu.make_async_copy(dxbuf.at[c], dx_ref.at[:, cols(c)], dxo.at[c])

    def dx_store(j):
        return pltpu.make_async_copy(obuf.at[j % 2], dx_ref.at[:, cols(n_done + j)], o_sem.at[j % 2])

    def each(n, fn):
        lax.fori_loop(0, n, lambda k, carry: (fn(k), carry)[1], 0)

    each(n_left, lambda j: w_load(j).start())
    each(n_done, lambda c: dx_load(c).start())
    each(n_chunk, lambda c: dw_load(c).start())

    def move(load, store, c):
        load(c).wait()
        store(c).start()

    def step(j, carry):
        w_load(j).wait()
        weight_stack(wbuf[j], stack)

        @pl.when(j >= 2)
        def _():
            dx_store(j - 2).wait()

        obuf[j % 2] = jnp.dot(
            cols_ref[...], stack[...], preferred_element_type=jnp.float32).astype(jnp.bfloat16)
        dx_store(j).start()

        @pl.when(j == 0)
        def _():
            each(n_done, lambda c: move(dx_load, dx_move, c))

        @pl.when(j == 1)
        def _():
            each(n_chunk, lambda c: move(dw_load, dw_store, c))

        return carry

    lax.fori_loop(0, n_left, step, 0)
    dx_store(n_left - 2).wait()
    dx_store(n_left - 1).wait()
    each(n_done, lambda c: dx_move(c).wait())
    each(n_chunk, lambda c: dw_store(c).wait())


def solution(mesh):
    cp_size = mesh.shape["cp"]
    dp_size = mesh.shape["dp"]

    def local_step(tokens, choices, router_w, expert_bias):
        pieces_n, seq, dim = tokens.shape
        rows_all = pieces_n * dp_size
        seq_all = seq * cp_size
        experts = router_w.shape[0]
        choice_num = choices.shape[2]
        tok_n = pieces_n * seq
        n_chunk = dim // COLS
        n_dx = n_chunk - 5
        f32, bf16 = jnp.float32, jnp.bfloat16
        dma, any_shape = pltpu.SemaphoreType.DMA, jax.ShapeDtypeStruct
        flat = tokens.reshape(tok_n, dim)

        expert_ids = jnp.arange(experts, dtype=jnp.int32)
        counts = jnp.sum((choices[..., None] == expert_ids).astype(f32), axis=(1, 2))
        counts = jnp.concatenate([counts, jnp.zeros_like(counts)], axis=0)
        scale = ALPHA * experts / (rows_all * choice_num * seq_all * seq_all)
        got = [pltpu.VMEM((n_chunk, experts >> (k + 1), COLS), f32) for k in range(LEVELS - 1)]
        got.append(pltpu.VMEM((n_chunk, experts >> (LEVELS - 1), COLS // 2), f32))
        dw_sum, dx_done, grad_cols, small_sum = pl.pallas_call(
            functools.partial(main_kernel, n_dx, pieces_n, scale),
            out_shape=(any_shape((n_chunk, experts, COLS), f32), any_shape((n_dx, tok_n, COLS), bf16),
                       any_shape((tok_n, 6 * experts), bf16), any_shape((8, experts), f32)),
            in_specs=[VMEM, ANY, ANY], out_specs=(ANY, ANY, ANY, VMEM),
            scratch_shapes=[
                pltpu.VMEM((n_chunk, experts, COLS), f32), pltpu.VMEM((n_chunk, experts, COLS), f32), *got,
                pltpu.VMEM((2, tok_n, COLS), bf16), pltpu.VMEM((2, experts, COLS), f32),
                pltpu.VMEM((6 * experts, COLS), bf16), pltpu.VMEM((experts, tok_n), f32),
                pltpu.VMEM((3 * experts, tok_n), bf16), pltpu.VMEM((tok_n, 6 * experts), bf16),
                pltpu.VMEM((3, 8, experts), f32), pltpu.VMEM((2, 8, experts), f32),
                pltpu.VMEM((LEVELS, 8, experts), f32), pltpu.VMEM((LEVELS, 8, experts), f32),
                dma((LEVELS, n_chunk)), dma((LEVELS, n_chunk)), dma((LEVELS, n_chunk)),
                dma((LEVELS, n_chunk)), dma((LEVELS,)), dma((LEVELS,)), dma((2,)), dma((2,)),
                dma((2,)), dma((2,)), dma((2,)), dma((n_chunk,)), dma],
            compiler_params=pltpu.CompilerParams(
                collective_id=0, has_side_effects=True, vmem_limit_bytes=60 << 20),
        )(counts, flat, router_w)

        grad_router, grad_tokens = pl.pallas_call(
            last_kernel,
            out_shape=(any_shape((experts, dim), f32), any_shape((tok_n, dim), bf16)),
            in_specs=[VMEM, ANY, ANY, ANY], out_specs=(ANY, ANY),
            scratch_shapes=[
                pltpu.VMEM((n_chunk - n_dx, experts, COLS), f32), pltpu.VMEM((6 * experts, COLS), bf16),
                pltpu.VMEM((2, tok_n, COLS), bf16), pltpu.VMEM((n_chunk, experts, COLS), f32),
                pltpu.VMEM((n_dx, tok_n, COLS), bf16),
                dma((n_chunk - n_dx,)), dma((2,)), dma((n_chunk,)), dma((n_chunk,)),
                dma((n_dx,)), dma((n_dx,))],
            compiler_params=pltpu.CompilerParams(vmem_limit_bytes=44 << 20),
        )(grad_cols, router_w, dw_sum, dx_done)

        bal_loss = small_sum[1, 0]
        load_gap = rows_all * seq_all * choice_num - experts * small_sum[0].astype(jnp.int32)
        new_bias = expert_bias + GAMMA * jnp.sign(load_gap).astype(f32)
        return bal_loss, grad_router, grad_tokens.reshape(tokens.shape), new_bias

    tok_spec = P("dp", "cp", None)
    return jax.shard_map(local_step, mesh=mesh, in_specs=(tok_spec, tok_spec, P(), P()), out_specs=(P(), P(), tok_spec, P()), check_vma=False)
```

```python
import functools

import jax
import jax.numpy as jnp
from jax import lax
from jax.experimental import pallas as pl
from jax.experimental.pallas import tpu as pltpu
from jax.sharding import PartitionSpec as P

ALPHA = 0.1
GAMMA = 0.001
MESH = pl.DeviceIdType.MESH
ANY = pl.BlockSpec(memory_space=pl.ANY)
VMEM = pl.BlockSpec(memory_space=pltpu.VMEM)
COLS = 512
LEVELS = 5
WAIT_RS = (2, 4, 6, 8, 10)
WAIT_AG = (20, 18, 16, 14, 12)


def pieces(val):
    hi = val.astype(jnp.bfloat16)
    rest = val - hi.astype(jnp.float32)
    mid = rest.astype(jnp.bfloat16)
    low = (rest - mid.astype(jnp.float32)).astype(jnp.bfloat16)
    return hi, mid, low


def weight_stack(w, stack, order=(0, 1, 0, 2, 1, 0)):
    experts = w.shape[0]
    parts = pieces(w)
    for k, which in enumerate(order):
        stack[pl.ds(k * experts, experts), :] = parts[which]


def main_kernel(n_dx, seqs, scale, cnt_ref, x_ref, w_ref, dw_ref, dx_ref, cols_ref, small_out,
                acc, full, got0, got1, got2, got3, got4, xbuf, wbuf, stack, scores, rows_ref,
                cnt_cur, cnt_got, small_cur, small_got,
                rs_send, rs_recv, ag_send, ag_recv, sm_send, sm_recv, cnt_send, cnt_recv,
                x_sem, w_sem, o_sem, d_sem):
    n_chunk, experts = acc.shape[0], acc.shape[1]
    tok_n = xbuf.shape[1]
    seq = tok_n // seqs
    z, dp = lax.axis_index("cp"), lax.axis_index("dp")
    core, xb, yb = dp % 2, (dp // 2) % 2, dp // 4
    zl, zh = z % 2, z // 2
    by_core = (z, dp + 1 - 2 * core)
    by_x = (z, dp + 2 - 4 * xb)
    by_y = (z, dp + 4 - 8 * yb)
    by_zl = (z + 1 - 2 * zl, dp)
    by_zh = (z + 2 - 4 * zh, dp)
    first = (z, dp + (1 - core) * (2 - 4 * xb) + core * (4 - 8 * yb))
    second = (z, dp + core * (2 - 4 * xb) + (1 - core) * (4 - 8 * yb))
    peers = (by_core, first, by_zl, second, by_zh)
    bits = (core, (1 - core) * xb + core * yb, zl, (1 - core) * yb + core * xb, zh)
    got = (got0, got1, got2, got3, got4)

    barrier = pltpu.get_barrier_semaphore()
    for peer in (by_core, by_x, by_y, by_zl, by_zh):
        pl.semaphore_signal(barrier, inc=1, device_id=peer, device_id_type=MESH)

    size, keep, away, base = experts, [], [], 0
    for level in range(LEVELS - 1):
        size //= 2
        keep.append((pl.multiple_of(base + bits[level] * size, 8), size, 0, COLS))
        away.append((pl.multiple_of(base + (1 - bits[level]) * size, 8), size, 0, COLS))
        base = base + bits[level] * size
    half = COLS // 2
    row = pl.multiple_of(base, 8)
    keep.append((row, size, pl.multiple_of(zh * half, 128), half))
    away.append((row, size, pl.multiple_of((1 - zh) * half, 128), half))

    def region(ref, c, where):
        r, n, k, m = where
        return ref.at[c, pl.ds(r, n), pl.ds(k, m)]

    def rs_copy(level, c):
        return pltpu.make_async_remote_copy(
            src_ref=region(acc, c, away[level]), dst_ref=got[level].at[c], send_sem=rs_send.at[level, c],
            recv_sem=rs_recv.at[level, c], device_id=peers[level], device_id_type=MESH)

    def ag_copy(level, c):
        return pltpu.make_async_remote_copy(
            src_ref=region(full, c, keep[level]), dst_ref=region(full, c, keep[level]), send_sem=ag_send.at[level, c],
            recv_sem=ag_recv.at[level, c], device_id=peers[level], device_id_type=MESH)

    def sm_copy(level):
        return pltpu.make_async_remote_copy(
            src_ref=small_cur.at[level], dst_ref=small_got.at[level], send_sem=sm_send.at[level],
            recv_sem=sm_recv.at[level], device_id=(by_core, by_x, by_zl, by_y, by_zh)[level],
            device_id_type=MESH)

    def cnt_copy(k):
        return pltpu.make_async_remote_copy(
            src_ref=cnt_cur.at[k], dst_ref=cnt_got.at[k], send_sem=cnt_send.at[k],
            recv_sem=cnt_recv.at[k], device_id=(by_zl, by_zh)[k], device_id_type=MESH)

    def x_load(c):
        return pltpu.make_async_copy(
            x_ref.at[:, pl.ds(pl.multiple_of(c * COLS, COLS), COLS)], xbuf.at[c % 2], x_sem.at[c % 2])

    def w_load(j):
        return pltpu.make_async_copy(
            w_ref.at[:, pl.ds(pl.multiple_of(j * COLS, COLS), COLS)], wbuf.at[j % 2], w_sem.at[j % 2])

    def dx_store(j):
        return pltpu.make_async_copy(xbuf.at[j % 2], dx_ref.at[j], o_sem.at[j % 2])

    def dw_store(c):
        return pltpu.make_async_copy(full.at[c], dw_ref.at[c], d_sem.at[c])

    x_load(0).start()
    x_load(1).start()
    w_load(0).start()
    w_load(1).start()
    cnt_cur[0] = cnt_ref[...]
    scores[...] = jnp.zeros_like(scores)
    pl.semaphore_wait(barrier, LEVELS)
    cnt_copy(0).start()

    def score_step(i, carry):
        w_load(i).wait()
        weight_stack(wbuf[i % 2], stack, (0, 1, 2))
        x_load(i).wait()
        for t in range(0, tok_n, COLS):
            out = lax.dot_general(
                stack[pl.ds(0, 3 * experts), :], xbuf[i % 2, pl.ds(t, COLS), :], (((1,), (1,)), ((), ())),
                preferred_element_type=jnp.float32)
            scores[:, pl.ds(t, COLS)] += out[:experts] + (out[experts:2 * experts] + out[2 * experts:])
        after = (i + 2) % n_chunk
        x_load(after).start()
        w_load(after).start()

        @pl.when(i == n_chunk // 2)
        def _():
            cnt_copy(0).wait_send()
            cnt_copy(0).wait_recv()
            cnt_cur[1] = cnt_cur[0] + cnt_got[0]
            cnt_copy(1).start()

        return carry

    lax.fori_loop(0, n_chunk, score_step, 0)
    cnt_copy(1).wait_send()
    cnt_copy(1).wait_recv()
    cnt_cur[2] = cnt_cur[1] + cnt_got[1]
    small_cur[0] = jnp.zeros_like(small_cur[0])

    def grad_step(r, carry):
        span = pl.ds(pl.multiple_of(r * seq, seq), seq)
        place = lax.broadcasted_iota(jnp.int32, (experts, experts), 0)
        diag = place == lax.broadcasted_iota(jnp.int32, (experts, experts), 1)
        weight = jnp.sum(jnp.where(diag, cnt_cur[2, pl.ds(r, 1), :], 0.0), axis=1, keepdims=True) * scale
        sig = jax.nn.sigmoid(scores[:, span])
        total = jnp.sum(sig, axis=0, keepdims=True)
        normed = sig / total
        mixed = jnp.sum(normed * weight, axis=0, keepdims=True)
        grad = (weight - mixed) * (sig * (1.0 - sig) / total)
        for k, part in enumerate(pieces(grad)):
            rows_ref[pl.ds(k * experts, experts), span] = part
        turned = pieces(grad.T)
        for k, which in enumerate((0, 0, 1, 0, 1, 2)):
            cols_ref[span, pl.ds(k * experts, experts)] = turned[which]
        loss = jnp.sum(mixed, axis=1, keepdims=True)
        row_id = lax.broadcasted_iota(jnp.int32, (8, experts), 0)
        loads = cnt_ref[pl.ds(r, 1), :]
        small_cur[0] += jnp.where(row_id == 0, loads, jnp.where(row_id == 1, loss, 0.0))
        return carry

    lax.fori_loop(0, seqs, grad_step, 0)

    def step(i, carry):
        def at(offset):
            c = i - offset
            return c, jnp.logical_and(c >= 0, c < n_chunk)

        for level in range(LEVELS):
            c, live = at(WAIT_AG[level])

            @pl.when(live)
            def _(level=level, c=c):
                copy = ag_copy(level, c)
                copy.wait_send()
                copy.wait_recv()
                if level > 0:
                    ag_copy(level - 1, c).start()
                else:
                    dw_store(c).start()

        for level in reversed(range(LEVELS)):
            c, live = at(WAIT_RS[level])

            @pl.when(live)
            def _(level=level, c=c):
                copy = rs_copy(level, c)
                copy.wait_send()
                copy.wait_recv()
                r, n, k, m = keep[level]
                total = acc[c, pl.ds(r, n), pl.ds(k, m)] + got[level][c]
                if level < LEVELS - 1:
                    acc[c, pl.ds(r, n), pl.ds(k, m)] = total
                    rs_copy(level + 1, c).start()
                else:
                    full[c, pl.ds(r, n), pl.ds(k, m)] = total
                    ag_copy(level, c).start()

        for level in range(LEVELS + 1):
            @pl.when(i == 2 * level)
            def _(level=level):
                if level > 0:
                    copy = sm_copy(level - 1)
                    copy.wait_send()
                    copy.wait_recv()
                    total = small_cur[level - 1] + small_got[level - 1]
                    if level < LEVELS:
                        small_cur[level] = total
                    else:
                        small_out[...] = total
                if level < LEVELS:
                    sm_copy(level).start()

        @pl.when(i < n_chunk)
        def _():
            x_load(i).wait()
            out = jnp.dot(rows_ref[...], xbuf[i % 2], preferred_element_type=jnp.float32)
            acc[i] = out[:experts] + (out[experts:2 * experts] + out[2 * experts:])
            rs_copy(0, i).start()

            @pl.when(i + 2 < n_chunk)
            def _():
                x_load(i + 2).start()

        @pl.when(jnp.logical_and(i >= n_chunk, i < n_chunk + n_dx))
        def _():
            j = i - n_chunk
            w_load(j).wait()
            weight_stack(wbuf[j % 2], stack)

            @pl.when(j + 2 < n_dx)
            def _():
                w_load(j + 2).start()

            @pl.when(j >= 2)
            def _():
                dx_store(j - 2).wait()

            xbuf[j % 2] = jnp.dot(
                cols_ref[...], stack[...], preferred_element_type=jnp.float32).astype(jnp.bfloat16)
            dx_store(j).start()

        return carry

    lax.fori_loop(0, n_chunk + WAIT_AG[0], step, 0)
    dx_store(n_dx - 2).wait()
    dx_store(n_dx - 1).wait()

    def finish(c, carry):
        dw_store(c).wait()
        return carry

    lax.fori_loop(0, n_chunk, finish, 0)


def last_kernel(cols_ref, w_ref, dw_in, dx_in, dw_ref, dx_ref,
                wbuf, stack, obuf, dwbuf, dxbuf, w_sem, o_sem, dwi, dwo, dxi, dxo):
    n_chunk, n_done = dw_in.shape[0], dx_in.shape[0]
    n_left = n_chunk - n_done

    def cols(c):
        return pl.ds(pl.multiple_of(c * COLS, COLS), COLS)

    def w_load(j):
        return pltpu.make_async_copy(w_ref.at[:, cols(n_done + j)], wbuf.at[j], w_sem.at[j])

    def dw_load(c):
        return pltpu.make_async_copy(dw_in.at[c], dwbuf.at[c], dwi.at[c])

    def dw_store(c):
        return pltpu.make_async_copy(dwbuf.at[c], dw_ref.at[:, cols(c)], dwo.at[c])

    def dx_load(c):
        return pltpu.make_async_copy(dx_in.at[c], dxbuf.at[c], dxi.at[c])

    def dx_move(c):
        return pltpu.make_async_copy(dxbuf.at[c], dx_ref.at[:, cols(c)], dxo.at[c])

    def dx_store(j):
        return pltpu.make_async_copy(obuf.at[j % 2], dx_ref.at[:, cols(n_done + j)], o_sem.at[j % 2])

    def each(n, fn):
        lax.fori_loop(0, n, lambda k, carry: (fn(k), carry)[1], 0)

    each(n_left, lambda j: w_load(j).start())
    each(n_done, lambda c: dx_load(c).start())
    each(n_chunk, lambda c: dw_load(c).start())

    def move(load, store, c):
        load(c).wait()
        store(c).start()

    def step(j, carry):
        w_load(j).wait()
        weight_stack(wbuf[j], stack)

        @pl.when(j >= 2)
        def _():
            dx_store(j - 2).wait()

        obuf[j % 2] = jnp.dot(
            cols_ref[...], stack[...], preferred_element_type=jnp.float32).astype(jnp.bfloat16)
        dx_store(j).start()

        @pl.when(j == 0)
        def _():
            each(n_done, lambda c: move(dx_load, dx_move, c))

        @pl.when(j == 1)
        def _():
            each(n_chunk, lambda c: move(dw_load, dw_store, c))

        return carry

    lax.fori_loop(0, n_left, step, 0)
    dx_store(n_left - 2).wait()
    dx_store(n_left - 1).wait()
    each(n_done, lambda c: dx_move(c).wait())
    each(n_chunk, lambda c: dw_store(c).wait())


def solution(mesh):
    cp_size = mesh.shape["cp"]
    dp_size = mesh.shape["dp"]

    def local_step(tokens, choices, router_w, expert_bias):
        pieces_n, seq, dim = tokens.shape
        rows_all = pieces_n * dp_size
        seq_all = seq * cp_size
        experts = router_w.shape[0]
        choice_num = choices.shape[2]
        tok_n = pieces_n * seq
        n_chunk = dim // COLS
        n_dx = n_chunk - 4
        f32, bf16 = jnp.float32, jnp.bfloat16
        dma, any_shape = pltpu.SemaphoreType.DMA, jax.ShapeDtypeStruct
        flat = tokens.reshape(tok_n, dim)

        expert_ids = jnp.arange(experts, dtype=jnp.int32)
        counts = jnp.sum((choices[..., None] == expert_ids).astype(f32), axis=(1, 2))
        counts = jnp.concatenate([counts, jnp.zeros_like(counts)], axis=0)
        scale = ALPHA * experts / (rows_all * choice_num * seq_all * seq_all)
        got = [pltpu.VMEM((n_chunk, experts >> (k + 1), COLS), f32) for k in range(LEVELS - 1)]
        got.append(pltpu.VMEM((n_chunk, experts >> (LEVELS - 1), COLS // 2), f32))
        dw_sum, dx_done, grad_cols, small_sum = pl.pallas_call(
            functools.partial(main_kernel, n_dx, pieces_n, scale),
            out_shape=(any_shape((n_chunk, experts, COLS), f32), any_shape((n_dx, tok_n, COLS), bf16),
                       any_shape((tok_n, 6 * experts), bf16), any_shape((8, experts), f32)),
            in_specs=[VMEM, ANY, ANY], out_specs=(ANY, ANY, VMEM, VMEM),
            scratch_shapes=[
                pltpu.VMEM((n_chunk, experts, COLS), f32), pltpu.VMEM((n_chunk, experts, COLS), f32), *got,
                pltpu.VMEM((2, tok_n, COLS), bf16), pltpu.VMEM((2, experts, COLS), f32),
                pltpu.VMEM((6 * experts, COLS), bf16), pltpu.VMEM((experts, tok_n), f32),
                pltpu.VMEM((3 * experts, tok_n), bf16),
                pltpu.VMEM((3, 8, experts), f32), pltpu.VMEM((2, 8, experts), f32),
                pltpu.VMEM((LEVELS, 8, experts), f32), pltpu.VMEM((LEVELS, 8, experts), f32),
                dma((LEVELS, n_chunk)), dma((LEVELS, n_chunk)), dma((LEVELS, n_chunk)),
                dma((LEVELS, n_chunk)), dma((LEVELS,)), dma((LEVELS,)), dma((2,)), dma((2,)),
                dma((2,)), dma((2,)), dma((2,)), dma((n_chunk,))],
            compiler_params=pltpu.CompilerParams(
                collective_id=0, has_side_effects=True, vmem_limit_bytes=47 << 20),
        )(counts, flat, router_w)

        grad_router, grad_tokens = pl.pallas_call(
            last_kernel,
            out_shape=(any_shape((experts, dim), f32), any_shape((tok_n, dim), bf16)),
            in_specs=[VMEM, ANY, ANY, ANY], out_specs=(ANY, ANY),
            scratch_shapes=[
                pltpu.VMEM((n_chunk - n_dx, experts, COLS), f32), pltpu.VMEM((6 * experts, COLS), bf16),
                pltpu.VMEM((2, tok_n, COLS), bf16), pltpu.VMEM((n_chunk, experts, COLS), f32),
                pltpu.VMEM((n_dx, tok_n, COLS), bf16),
                dma((n_chunk - n_dx,)), dma((2,)), dma((n_chunk,)), dma((n_chunk,)),
                dma((n_dx,)), dma((n_dx,))],
            compiler_params=pltpu.CompilerParams(vmem_limit_bytes=38 << 20),
        )(grad_cols, router_w, dw_sum, dx_done)

        bal_loss = small_sum[1, 0]
        load_gap = rows_all * seq_all * choice_num - experts * small_sum[0].astype(jnp.int32)
        new_bias = expert_bias + GAMMA * jnp.sign(load_gap).astype(f32)
        return bal_loss, grad_router, grad_tokens.reshape(tokens.shape), new_bias

    tok_spec = P("dp", "cp", None)
    return jax.shard_map(local_step, mesh=mesh, in_specs=(tok_spec, tok_spec, P(), P()), out_specs=(P(), P(), tok_spec, P()), check_vma=False)
```
